32 devices in a mesh: grp: 2 (over y), exp: 4 (over z), tp: 4 (over x, core).
Axes of the slice: x: 2, y: 2, z: 4, core: 2. Of those that a mesh axis runs over, the one named last changes fastest.
Arguments:
- tokens: bfloat16 [128, 3584], P(('grp', 'exp'), 'tp'), parts along dimension 0, may hold values from -6 to 6
- gate_up_weight: bfloat16 [3584, 2, 18944], P('tp', None, 'exp'), may hold values from -0.09375 to 0.09375
- down_weight: bfloat16 [18944, 3584], P('exp', 'tp'), may hold values from -0.046875 to 0.046875
- adapter_in: bfloat16 [4, 3584, 16], P('exp', 'tp'), may hold values from -0.09375 to 0.09375
- adapter_out: bfloat16 [4, 16, 3584], P('exp', None, 'tp'), may hold values from -1.5 to 1.5
- expert_ids: int32 [128, 2], P(('grp', 'exp')), parts along dimension 0, may hold values from 0 to 3, all different within a row; in each aligned block of 16 rows (0 to 15, 16 to 31, ...) at most 16 rows name the same one
- route_weight: float32 [128, 2], P(('grp', 'exp')), parts along dimension 0, may hold values from 0.2 to 1
Outputs:
- mixed: bfloat16 [128, 3584], P(('grp', 'exp'), 'tp'), parts along dimension 0
The draws below stay inside these ranges and needn't reach their ends.
There are 2 independent parts, one for each index of `grp`. The reference program is written for one: setup_inputs(seed, part) draws one part's arguments, and reference() takes and returns one part's arrays. A program takes and returns all parts, laid end to end along the dimension named above; an argument that names none is the same for every part. Nothing has to cross between parts.
Inputs may be any that keep to these rules, and one draw needn't show every extreme that they name: `expert_ids`: each row names 2 different experts. Among the 16 rows of one index of exp (aligned blocks of 16 rows) no expert is named by more than 16 rows, and in every draw some expert is named by exactly 16 rows of some block.
All inputs are finite; a program needn't handle non-finite values.
Results may differ from the reference program's by a relative error of at most 0.025.
Values may be sent and summed in bfloat16 or wider, within the bound.
A program may use at most 64 MiB of HBM per device.

```python
import math
import jax
import jax.numpy as jnp
import numpy as np
from jax import lax

D = 3584
FF = 18944
RANK = 16
TOP = 2
TOK_DEV = 16
EXPERTS = 4
TOKENS = 64
CAP = 16
N_EXP = 4
N_TP = 4


def steps_of(key, dims, cuts, least, top_value):
    level, own = 1.0, jax.random.fold_in(key, 6)
    for dim, shards_of in cuts:
        heights = jnp.exp(jax.random.uniform(jax.random.fold_in(own, dim), (shards_of,), jnp.float32, least / len(cuts), top_value / len(cuts)))
        level = level * jnp.repeat(heights, dims[dim] // shards_of).reshape([-1 if axis == dim else 1 for axis in range(len(dims))])
    return level


def assign_block(key, own, number, rows, count, top, reach, skew):
    sequence = jax.random.permutation(key, count)
    crowded, common = portions_of(count, rows * top, reach, skew, True), portions_of(count, rows * top, reach, skew, False)
    places = jnp.arange(count)

    def named(lengths, turn):
        used = int((lengths > 0).sum())
        fixed = max(1, used // 4)
        shifted = fixed + (places - fixed + turn * (used - fixed)) % max(1, count - fixed)
        return jnp.zeros((count,), jnp.int32).at[sequence[jnp.where(places < fixed, places, shifted)]].set(jnp.asarray(lengths, jnp.int32))

    lengths = jnp.where(number % 4 == 0, named(crowded, number // 4), named(common, number - number // 4 - 1))
    mixed = jax.random.permutation(jax.random.fold_in(own, 3), count)
    donor, taker = mixed[0:count // 2 * 2:2], mixed[1:count // 2 * 2:2]
    margin = jnp.minimum(lengths[donor] - 1, reach - lengths[taker]) // 2
    margin = jnp.where((donor == sequence[0]) | (taker == sequence[0]) | (lengths[taker] == 0), 0, jnp.maximum(margin, 0))
    shifted = jax.random.randint(jax.random.fold_in(own, 4), (count // 2,), 0, 1 << 20) % (margin + 1)
    lengths = lengths.at[donor].add(-shifted).at[taker].add(shifted)
    members = jnp.searchsorted(jnp.cumsum(lengths), jnp.arange(rows * top), side="right").astype(jnp.int32)
    listing = members.reshape(top, rows).T
    listing = listing[jax.random.permutation(jax.random.fold_in(own, 1), rows)]
    turn = jax.random.randint(jax.random.fold_in(own, 2), (rows, 1), 0, top)
    return jnp.take_along_axis(listing, (jnp.arange(top)[None, :] + turn) % top, axis=1)


def portions_of(count, total, bound, slope, full):
    portions = [(1 << 20) // math.isqrt(rank ** slope) + 1 for rank in range(1, count + 1)]
    largest = bound if full else min(bound, max(-(-total // count), total * portions[0] // sum(portions)))
    least = 1 if total - largest >= count - 1 else 0
    holding, spare = [largest] + [least] * (count - 1), total - largest - least * (count - 1)
    while spare > 0:
        candidates = [i for i in range(1, count) if holding[i] < largest] or [i for i in range(1, count) if holding[i] < bound]
        whole, remaining = sum([portions[i] for i in candidates]), spare
        for i in candidates:
            more = min(bound - holding[i], max(1, remaining * portions[i] // whole), spare)
            holding[i] = holding[i] + more
            spare = spare - more
    return np.array(holding)


def scatter_about(own_key, shape, width, most, cuts=(), kind=jnp.bfloat16):
    level = steps_of(own_key, shape, cuts, -0.22, 0.18) if cuts else 1.0
    result = jax.random.normal(own_key, shape, jnp.float32) * width * level
    return jnp.minimum(jnp.maximum(result, -most), most).astype(kind)


def setup_inputs(seed: int = 0, part: int = 0) -> dict:
    keys = jax.random.split(jax.random.key(seed), 8)
    part_splits = jax.random.split(jax.random.fold_in(keys[7], part), 8)
    tokens = scatter_about(part_splits[0], (TOKENS, D), 1.0, 6.0, ((0, 4), (1, 4)))
    gate_up_weight = scatter_about(keys[1], (D, 2, FF), D ** -0.5, 0.09375, ((0, 4), (2, 4)))
    down_weight = scatter_about(keys[2], (FF, D), FF ** -0.5, 0.046875, ((0, 4), (1, 4)))
    adapter_in = scatter_about(keys[3], (EXPERTS, D, RANK), D ** -0.5, 0.09375, ((0, 4), (1, 4)))
    adapter_out = scatter_about(keys[4], (EXPERTS, RANK, D), RANK ** -0.5, 1.5, ((0, 4), (2, 4)))
    expert_ids_keys = jax.random.split(jax.random.fold_in(part_splits[5], 1), TOKENS // TOK_DEV)
    expert_ids_turns = jax.random.permutation(jax.random.fold_in(part_splits[5], 3), TOKENS // TOK_DEV)
    expert_ids = jax.vmap(lambda own, number: assign_block(jax.random.fold_in(part_splits[5], 2), own, number, TOK_DEV, EXPERTS, TOP, CAP, 2))(expert_ids_keys, expert_ids_turns).reshape((TOKENS, TOP))
    route_weight = jnp.clip(0.2 + 0.8 * jax.random.uniform(part_splits[6], (TOKENS, TOP), jnp.float32) ** steps_of(part_splits[6], (TOKENS, TOP), ((0, 4),), -0.2, 0.2), 0.2, 1.0)
    return dict(tokens=tokens, gate_up_weight=gate_up_weight, down_weight=down_weight, adapter_in=adapter_in, adapter_out=adapter_out, expert_ids=expert_ids, route_weight=route_weight)


def reference(tokens, gate_up_weight, down_weight, adapter_in, adapter_out, expert_ids, route_weight):
    token_count = tokens.shape[0]
    feat_width = D // N_TP
    pair = jnp.zeros((token_count, 2 * FF), jnp.float32)
    for block_index in range(N_TP):
        lower = block_index * feat_width
        block_weight = gate_up_weight[lower:lower + feat_width].reshape(feat_width, 2 * FF)
        partial_sum = jnp.dot(tokens[:, lower:lower + feat_width], block_weight, preferred_element_type=jnp.float32)
        rounded = lax.optimization_barrier(partial_sum.astype(jnp.bfloat16))
        pair = pair + rounded.astype(jnp.float32)
    gate = pair[:, :FF]
    up_part = pair[:, FF:]
    hidden = (jax.nn.silu(gate) * up_part).astype(jnp.bfloat16)
    hidden_width = FF // N_EXP
    base_out = jnp.zeros((token_count, D), jnp.float32)
    for block_index in range(N_EXP):
        lower = block_index * hidden_width
        partial_sum = jnp.dot(hidden[:, lower:lower + hidden_width], down_weight[lower:lower + hidden_width], preferred_element_type=jnp.float32)
        rounded = lax.optimization_barrier(partial_sum.astype(jnp.bfloat16))
        base_out = base_out + rounded.astype(jnp.float32)
    expert_count = adapter_in.shape[0]
    in_flat = jnp.transpose(adapter_in, (1, 0, 2)).reshape(D, expert_count * RANK)
    rank_mid = jnp.dot(tokens, in_flat, preferred_element_type=jnp.float32).astype(jnp.bfloat16)
    rank_mid = rank_mid.reshape(token_count, expert_count, RANK)
    hits = (expert_ids[:, :, None] == jnp.arange(expert_count, dtype=jnp.int32)[None, None, :]).astype(jnp.float32)
    coefficient = jnp.sum(hits * route_weight[:, :, None], axis=1)

    def add_expert(total, pieces):
        mid_piece, out_map, coef_column = pieces
        expert_out = jnp.dot(mid_piece, out_map, preferred_element_type=jnp.float32).astype(jnp.bfloat16)
        return total + coef_column[:, None] * expert_out.astype(jnp.float32), None

    adapter_sum, _ = lax.scan(add_expert, jnp.zeros((token_count, D), jnp.float32),
                              (jnp.transpose(rank_mid, (1, 0, 2)), adapter_out, coefficient.T))
    return (base_out + adapter_sum).astype(jnp.bfloat16)
```

```python
import functools
import jax
import jax.numpy as jnp
from jax import lax
from jax.experimental import pallas as pl
from jax.experimental.pallas import tpu as pltpu
from jax.sharding import PartitionSpec as P

LANES = 128
CHUNK_TILES = 8
MESH = pl.DeviceIdType.MESH
BF16, F32 = jnp.bfloat16, jnp.float32


def chunks_of(tiles):
    spans, first = [], 0
    while first < tiles:
        count = min(CHUNK_TILES, tiles - first)
        spans.append((first, count))
        first += count
    return spans


def kernel(
    exp_count, tok_ref, gu_ref, down_ref, ain_ref, aout_ref, ids_ref, weight_ref, out_ref,
    gu, down, tok_all, coef_all, coef_own, lhs, ain_pad, aout_pad,
    keep1, send1, recv1, keep2, send2, recv2, hid, total, send_f, recv_f,
    gu_sem, down_sem, tok_send, tok_recv, coef_send, coef_recv,
    s1_send, s1_recv, s2_send, s2_recv, hp_send, hp_recv, hx_send, hx_recv, hr_send, hr_recv,
    f_send, f_recv,
):
    me = lax.axis_index("exp")
    tp = lax.axis_index("tp")
    own_rows, feat = tok_ref.shape
    hidden = gu_ref.shape[2]
    rank = ain_ref.shape[2]
    tiles = hidden // LANES
    spans = chunks_of(tiles)
    last = len(spans) - 1
    core, side = tp % 2, tp // 2
    partner = side * 2 + (1 - core)
    across = (1 - side) * 2 + core
    blocks = [
        core * 2 + side,
        core * 2 + (1 - side),
        (1 - core) * 2 + side,
        (1 - core) * 2 + (1 - side),
    ]
    mine, crossed = blocks[0], blocks[1]

    def gu_copy(t):
        cols = pl.ds(pl.multiple_of(t * LANES, LANES), LANES)
        return pltpu.make_async_copy(gu_ref.at[:, :, cols], gu.at[t], gu_sem.at[t])

    def down_copy(j):
        first, count = spans[j]
        rows = pl.ds(first * LANES, count * LANES)
        return pltpu.make_async_copy(down_ref.at[rows], down.at[rows], down_sem.at[j])

    def start_gu(t, carry):
        gu_copy(t).start()
        return carry

    lax.fori_loop(0, tiles, start_gu, 0)
    for j in range(len(spans)):
        down_copy(j).start()

    barrier = pltpu.get_barrier_semaphore()
    for d in range(1, exp_count):
        pl.semaphore_signal(
            barrier, inc=1, device_id={"exp": (me + d) % exp_count}, device_id_type=MESH
        )
    for peer in (partner, across):
        pl.semaphore_signal(barrier, inc=1, device_id={"tp": peer}, device_id_type=MESH)

    lane = lax.broadcasted_iota(jnp.int32, (own_rows, LANES), 1)
    coef = jnp.zeros((own_rows, LANES), F32)
    for k in range(ids_ref.shape[1]):
        coef = coef + jnp.where(lane == ids_ref[:, k:k + 1], weight_ref[:, k:k + 1], 0.0)
    coef_own[...] = coef
    coef_all[me] = coef
    tok_all[me] = tok_ref[...]
    ain_pad[...] = jnp.zeros_like(ain_pad)
    ain_pad[:, :rank] = ain_ref[0]
    aout_pad[...] = jnp.zeros_like(aout_pad)
    aout_pad[:rank, :] = aout_ref[0]

    pl.semaphore_wait(barrier, exp_count + 1)

    def exp_copy(src, dst, send, recv, d):
        return pltpu.make_async_remote_copy(
            src_ref=src, dst_ref=dst, send_sem=send.at[d - 1], recv_sem=recv.at[d - 1],
            device_id={"exp": (me + d) % exp_count}, device_id_type=MESH,
        )

    tok_copies = [
        exp_copy(tok_ref, tok_all.at[me], tok_send, tok_recv, d) for d in range(1, exp_count)
    ]
    coef_copies = [
        exp_copy(coef_own, coef_all.at[me], coef_send, coef_recv, d) for d in range(1, exp_count)
    ]
    for copy in tok_copies + coef_copies:
        copy.start()

    def span_cols(j):
        first, count = spans[j]
        return pl.ds(first * LANES, (count + (j == last)) * LANES)

    def tp_copy(src, dst, send, recv, j, peer):
        return pltpu.make_async_remote_copy(
            src_ref=src, dst_ref=dst, send_sem=send.at[j], recv_sem=recv.at[j],
            device_id={"tp": peer}, device_id_type=MESH,
        )

    def s1_copy(j):
        cols = span_cols(j)
        return tp_copy(send1.at[:, cols], recv1.at[:, cols], s1_send, s1_recv, j, partner)

    def s2_copy(j):
        cols = span_cols(j)
        return tp_copy(send2.at[:, cols], recv2.at[:, cols], s2_send, s2_recv, j, across)

    def hp_copy(j):
        ref = hid.at[mine, :, span_cols(j)]
        return tp_copy(ref, ref, hp_send, hp_recv, j, partner)

    def hx_copy(j):
        ref = hid.at[mine, :, span_cols(j)]
        return tp_copy(ref, ref, hx_send, hx_recv, j, across)

    def hr_copy(j):
        ref = hid.at[crossed, :, span_cols(j)]
        return tp_copy(ref, ref, hr_send, hr_recv, j, partner)

    for copy in tok_copies:
        copy.wait_recv()

    row = lax.broadcasted_iota(jnp.int32, (LANES, 4 * LANES), 0)
    col = lax.broadcasted_iota(jnp.int32, (LANES, 4 * LANES), 1)
    spread = jnp.where(col % (2 * LANES) == 2 * row + col // (2 * LANES), 1.0, 0.0).astype(BF16)
    ordered = jnp.concatenate([tok_all[b] for b in blocks], axis=0)
    rows = ordered.shape[0]
    stacked = jnp.concatenate(
        [ordered[:, k * LANES:(k + 1) * LANES] for k in range(feat // LANES)], axis=0
    )
    wide = jnp.dot(stacked, spread, preferred_element_type=F32).astype(BF16)
    for k in range(feat // LANES):
        for p in range(4):
            for s in range(2):
                lhs[
                    (2 * p + s) * own_rows:(2 * p + s + 1) * own_rows,
                    2 * k * LANES:2 * (k + 1) * LANES,
                ] = wide[
                    k * rows + p * own_rows:k * rows + (p + 1) * own_rows,
                    2 * s * LANES:2 * (s + 1) * LANES,
                ]

    half = 4 * own_rows

    def store_pair(cols, value):
        keep1[:, cols] = value[:half]
        send1[:, cols] = value[half:].astype(BF16)

    def weight_tile(t):
        return gu.at[t].reshape(2 * feat, LANES)[...]

    def product(j):
        first, count = spans[j]

        def two(i, carry):
            t = first + 2 * i
            gu_copy(t).wait()
            gu_copy(t + 1).wait()
            weight = jnp.concatenate([weight_tile(t), weight_tile(t + 1)], axis=1)
            value = jnp.dot(lhs[...], weight, preferred_element_type=F32)
            store_pair(pl.ds(pl.multiple_of(t * LANES, LANES), 2 * LANES), value)
            return carry

        lax.fori_loop(0, count // 2, two, 0)
        if count % 2:
            t = first + count - 1
            gu_copy(t).wait()
            value = jnp.dot(lhs[...], weight_tile(t), preferred_element_type=F32)
            store_pair(pl.ds(t * LANES, LANES), value)
        s1_copy(j).start()

    def rank_product():
        value = jnp.dot(ordered, ain_pad[...], preferred_element_type=F32)
        blank = jnp.zeros((own_rows, LANES), F32)
        parts = []
        for p in range(4):
            parts += [value[p * own_rows:(p + 1) * own_rows], blank]
        store_pair(pl.ds(hidden, LANES), jnp.concatenate(parts, axis=0))

    def reduce_near(j):
        s1_copy(j).wait_recv()
        cols = span_cols(j)
        value = keep1[:, cols] + recv1[:, cols].astype(F32)
        keep2[:, cols] = value[:2 * own_rows]
        send2[:, cols] = value[2 * own_rows:].astype(BF16)
        s2_copy(j).start()

    def activate(j):
        s2_copy(j).wait_recv()
        first, count = spans[j]
        cols = pl.ds(first * LANES, count * LANES)
        pair = keep2[:, cols] + recv2[:, cols].astype(F32)
        hid[mine, :, cols] = (jax.nn.silu(pair[:own_rows]) * pair[own_rows:]).astype(BF16)
        if j == last:
            cols = pl.ds(hidden, LANES)
            pair = keep2[:own_rows, cols] + recv2[:own_rows, cols].astype(F32)
            hid[mine, :, cols] = pair.astype(BF16)
        hx_copy(j).start()
        hp_copy(j).start()

    def relay(j):
        hx_copy(j).wait_recv()
        hr_copy(j).start()

    def project(j):
        hp_copy(j).wait_recv()
        hr_copy(j).wait_recv()
        down_copy(j).wait()
        first, count = spans[j]
        cols = pl.ds(first * LANES, count * LANES)
        value = jnp.dot(
            hid[:, :, cols].reshape(rows, count * LANES), down[cols, :],
            preferred_element_type=F32,
        )
        if j == 0:
            total[...] = value
        else:
            total[...] += value

    chunk_count = len(spans)
    for j in range(chunk_count):
        product(j)
        if j == 0:
            rank_product()
        else:
            reduce_near(j - 1)
        if j >= 4:
            activate(j - 4)
    reduce_near(last)
    done = max(0, chunk_count - 4)
    for j in range(done, chunk_count):
        activate(j)
        if j >= 2:
            relay(j - 2)
        if j >= 3:
            project(j - 3)
    for j in range(max(0, chunk_count - 2), chunk_count):
        relay(j)
    for j in range(max(0, chunk_count - 3), chunk_count):
        project(j)

    for copy in coef_copies:
        copy.wait_recv()
    rank_mid = hid[:, :, pl.ds(hidden, LANES)].reshape(rows, LANES)
    expert_out = jnp.dot(rank_mid, aout_pad[...], preferred_element_type=F32).astype(BF16)
    all_coef = coef_all[...].reshape(rows, LANES)
    wide_lane = lax.broadcasted_iota(jnp.int32, (rows, LANES), 1)
    column = jnp.sum(jnp.where(wide_lane == me, all_coef, 0.0), axis=1, keepdims=True)
    part = total[...] + column * expert_out.astype(F32)
    total[...] = part
    send_f[...] = part.astype(BF16).reshape(exp_count, own_rows, feat)
    f_copies = [
        exp_copy(send_f.at[(me + d) % exp_count], recv_f.at[d - 1], f_send, f_recv, d)
        for d in range(1, exp_count)
    ]
    for copy in f_copies:
        copy.start()
    result = total[pl.ds(pl.multiple_of(me * own_rows, own_rows), own_rows), :]
    for copy, d in zip(f_copies, range(1, exp_count)):
        copy.wait_recv()
        result = result + recv_f[d - 1].astype(F32)
    out_ref[...] = result.astype(out_ref.dtype)

    for copy in tok_copies + coef_copies + f_copies:
        copy.wait_send()
    for j in range(chunk_count):
        for make in (s1_copy, s2_copy, hp_copy, hx_copy, hr_copy):
            make(j).wait_send()


def fused(tokens, gate_up_weight, down_weight, adapter_in, adapter_out, expert_ids, route_weight):
    exp_count = lax.axis_size("exp")
    own_rows, feat = tokens.shape
    hidden = gate_up_weight.shape[2]
    tiles = hidden // LANES
    chunk_count = len(chunks_of(tiles))
    wide = hidden + LANES
    rows = exp_count * own_rows
    vmem = functools.partial(pltpu.VMEM)
    dma = lambda n: pltpu.SemaphoreType.DMA((n,))
    peers = exp_count - 1
    in_vmem = pl.BlockSpec(memory_space=pltpu.VMEM)
    in_place = pl.BlockSpec(memory_space=pl.ANY)
    return pl.pallas_call(
        functools.partial(kernel, exp_count),
        out_shape=jax.ShapeDtypeStruct((own_rows, feat), BF16),
        in_specs=[in_vmem, in_place, in_place, in_vmem, in_vmem, in_vmem, in_vmem],
        out_specs=in_vmem,
        scratch_shapes=[
            vmem((tiles, feat, 2, LANES), BF16),
            vmem((hidden, feat), BF16),
            vmem((exp_count, own_rows, feat), BF16),
            vmem((exp_count, own_rows, LANES), F32),
            vmem((own_rows, LANES), F32),
            vmem((2 * rows, 2 * feat), BF16),
            vmem((feat, LANES), BF16),
            vmem((LANES, feat), BF16),
            vmem((4 * own_rows, wide), F32),
            vmem((4 * own_rows, wide), BF16),
            vmem((4 * own_rows, wide), BF16),
            vmem((2 * own_rows, wide), F32),
            vmem((2 * own_rows, wide), BF16),
            vmem((2 * own_rows, wide), BF16),
            vmem((4, own_rows, wide), BF16),
            vmem((rows, feat), F32),
            vmem((exp_count, own_rows, feat), BF16),
            vmem((peers, own_rows, feat), BF16),
            dma(tiles), dma(chunk_count),
            dma(peers), dma(peers), dma(peers), dma(peers),
            *[dma(chunk_count) for _ in range(10)],
            dma(peers), dma(peers),
        ],
        compiler_params=pltpu.CompilerParams(
            collective_id=0, has_side_effects=True, vmem_limit_bytes=60 * 2**20
        ),
    )(tokens, gate_up_weight, down_weight, adapter_in, adapter_out, expert_ids, route_weight)


def plain(tokens, gate_up_weight, down_weight, adapter_in, adapter_out, expert_ids, route_weight):
    exp_count = lax.axis_size("exp")
    own_rows, feat_width = tokens.shape
    all_tokens = lax.all_gather(tokens, "exp", axis=0, tiled=True)
    hidden_width = gate_up_weight.shape[2]
    pair_weight = gate_up_weight.reshape(feat_width, 2 * hidden_width)
    pair_share = lax.psum_scatter(
        jnp.dot(all_tokens, pair_weight, preferred_element_type=jnp.float32).astype(jnp.bfloat16),
        "tp",
        scatter_dimension=0,
        tiled=True,
    ).astype(jnp.float32)
    hidden_share = (
        jax.nn.silu(pair_share[:, :hidden_width]) * pair_share[:, hidden_width:]
    ).astype(jnp.bfloat16)
    hidden = lax.all_gather(hidden_share, "tp", axis=0, tiled=True)
    base_out = lax.psum_scatter(
        jnp.dot(hidden, down_weight, preferred_element_type=jnp.float32).astype(jnp.bfloat16),
        "exp",
        scatter_dimension=0,
        tiled=True,
    ).astype(jnp.float32)
    top_count = expert_ids.shape[1]
    expert_count = adapter_in.shape[0] * exp_count
    flat_ids = expert_ids.reshape(own_rows * top_count)
    flat_weight = route_weight.reshape(own_rows * top_count)
    expert_hits = (flat_ids[:, None] == jnp.arange(expert_count, dtype=jnp.int32)[None, :]).astype(
        jnp.int32
    )
    capacity = max(2, 2 * top_count * own_rows // expert_count)
    slot_index = jnp.sum((jnp.cumsum(expert_hits, axis=0) - expert_hits) * expert_hits, axis=1)
    slot_target = flat_ids * capacity + slot_index
    slot_hits = (
        slot_target[:, None] == jnp.arange(expert_count * capacity, dtype=jnp.int32)[None, :]
    )
    combine_matrix = jnp.sum(
        (slot_hits.astype(jnp.float32) * flat_weight[:, None]).reshape(
            own_rows, top_count, expert_count * capacity
        ),
        axis=1,
    )
    dispatch_matrix = slot_hits.T.astype(jnp.bfloat16)
    repeated = jnp.repeat(tokens, top_count, axis=0)
    outgoing = jnp.dot(dispatch_matrix, repeated, preferred_element_type=jnp.float32).astype(
        jnp.bfloat16
    )
    outgoing = outgoing.reshape(expert_count, capacity, feat_width)
    rank_partial = jnp.einsum(
        "scd,dr->scr",
        lax.all_to_all(outgoing, "exp", split_axis=0, concat_axis=0, tiled=True),
        adapter_in[0],
        preferred_element_type=jnp.float32,
    )
    rank_mid = lax.psum(rank_partial, "tp").astype(jnp.bfloat16)
    expert_out = jnp.einsum(
        "scr,rd->scd", rank_mid, adapter_out[0], preferred_element_type=jnp.float32
    ).astype(jnp.bfloat16)
    returned = lax.all_to_all(expert_out, "exp", split_axis=0, concat_axis=0, tiled=True)
    adapter_sum = jnp.dot(
        combine_matrix,
        returned.reshape(expert_count * capacity, feat_width).astype(jnp.float32),
        precision=lax.Precision.HIGHEST,
        preferred_element_type=jnp.float32,
    )
    return (base_out + adapter_sum).astype(jnp.bfloat16)


def local(tokens, gate_up_weight, *rest):
    own_rows, feat = tokens.shape
    fits = (
        lax.axis_size("tp") == 4
        and lax.axis_size("exp") == 4
        and rest[1].shape[0] == 1
        and rest[1].shape[2] <= LANES
        and own_rows % 16 == 0
        and feat % LANES == 0
        and gate_up_weight.shape[2] % LANES == 0
    )
    return (fused if fits else plain)(tokens, gate_up_weight, *rest)


def solution(mesh):
    in_specs = (
        P(("grp", "exp"), "tp"),
        P("tp", None, "exp"),
        P("exp", "tp"),
        P("exp", "tp", None),
        P("exp", None, "tp"),
        P(("grp", "exp"), None),
        P(("grp", "exp"), None),
    )
    out_specs = P(("grp", "exp"), "tp")
    return jax.shard_map(local, mesh=mesh, in_specs=in_specs, out_specs=out_specs, check_vma=False)
```

```python
import functools
import jax
import jax.numpy as jnp
from jax import lax
from jax.experimental import pallas as pl
from jax.experimental.pallas import tpu as pltpu
from jax.sharding import PartitionSpec as P

LANES = 128
CHUNK_TILES = 8
MESH = pl.DeviceIdType.MESH
BF16, F32 = jnp.bfloat16, jnp.float32


def chunks_of(tiles):
    spans, first = [], 0
    while first < tiles:
        count = min(CHUNK_TILES, tiles - first)
        spans.append((first, count))
        first += count
    return spans


def kernel(
    exp_count, tok_ref, gu_ref, down_ref, ain_ref, aout_ref, ids_ref, weight_ref, out_ref,
    gu, down, tok_all, coef_all, coef_own, lhs, ain_pad, aout_pad,
    keep1, send1, recv1, keep2, send2, recv2, hid, total, send_f, recv_f,
    gu_sem, down_sem, tok_send, tok_recv, coef_send, coef_recv,
    s1_send, s1_recv, s2_send, s2_recv, hp_send, hp_recv, hx_send, hx_recv, hr_send, hr_recv,
    f_send, f_recv,
):
    me = lax.axis_index("exp")
    tp = lax.axis_index("tp")
    own_rows, feat = tok_ref.shape
    hidden = gu_ref.shape[2]
    rank = ain_ref.shape[1]
    tiles = hidden // LANES
    spans = chunks_of(tiles)
    last = len(spans) - 1
    core, side = tp % 2, tp // 2
    partner = side * 2 + (1 - core)
    across = (1 - side) * 2 + core
    blocks = [
        core * 2 + side,
        core * 2 + (1 - side),
        (1 - core) * 2 + side,
        (1 - core) * 2 + (1 - side),
    ]
    mine, crossed = blocks[0], blocks[1]

    def gu_copy(t):
        cols = pl.ds(pl.multiple_of(t * LANES, LANES), LANES)
        return pltpu.make_async_copy(gu_ref.at[:, :, cols], gu.at[t], gu_sem.at[t])

    def down_copy(j):
        first, count = spans[j]
        rows = pl.ds(first * LANES, count * LANES)
        return pltpu.make_async_copy(down_ref.at[rows], down.at[rows], down_sem.at[j])

    def start_gu(t, carry):
        gu_copy(t).start()
        return carry

    lax.fori_loop(0, tiles, start_gu, 0)
    for j in range(len(spans)):
        down_copy(j).start()

    barrier = pltpu.get_barrier_semaphore()
    for d in range(1, exp_count):
        pl.semaphore_signal(
            barrier, inc=1, device_id={"exp": (me + d) % exp_count}, device_id_type=MESH
        )
    for peer in (partner, across):
        pl.semaphore_signal(barrier, inc=1, device_id={"tp": peer}, device_id_type=MESH)

    lane = lax.broadcasted_iota(jnp.int32, (own_rows, LANES), 1)
    diagonal = lax.broadcasted_iota(
        jnp.int32, (own_rows, own_rows), 0
    ) == lax.broadcasted_iota(jnp.int32, (own_rows, own_rows), 1)

    def column_of(line):
        return jnp.sum(jnp.where(diagonal, line, 0.0), axis=1, keepdims=True)

    coef = jnp.zeros((own_rows, LANES), F32)
    for k in range(ids_ref.shape[0]):
        named = column_of(ids_ref[k:k + 1, :].astype(F32)).astype(jnp.int32)
        coef = coef + jnp.where(lane == named, column_of(weight_ref[k:k + 1, :]), 0.0)
    coef_own[...] = coef
    coef_all[me] = coef
    tok_all[me] = tok_ref[...]
    ain_pad[...] = jnp.zeros_like(ain_pad)
    ain_pad[:rank, :] = ain_ref[0]
    aout_pad[...] = jnp.zeros_like(aout_pad)
    aout_pad[:rank, :] = aout_ref[0]

    pl.semaphore_wait(barrier, exp_count + 1)

    def exp_copy(src, dst, send, recv, d):
        return pltpu.make_async_remote_copy(
            src_ref=src, dst_ref=dst, send_sem=send.at[d - 1], recv_sem=recv.at[d - 1],
            device_id={"exp": (me + d) % exp_count}, device_id_type=MESH,
        )

    tok_copies = [
        exp_copy(tok_ref, tok_all.at[me], tok_send, tok_recv, d) for d in range(1, exp_count)
    ]
    coef_copies = [
        exp_copy(coef_own, coef_all.at[me], coef_send, coef_recv, d) for d in range(1, exp_count)
    ]
    for copy in tok_copies + coef_copies:
        copy.start()

    def span_cols(j):
        first, count = spans[j]
        return pl.ds(first * LANES, (count + (j == last)) * LANES)

    def tp_copy(src, dst, send, recv, j, peer):
        return pltpu.make_async_remote_copy(
            src_ref=src, dst_ref=dst, send_sem=send.at[j], recv_sem=recv.at[j],
            device_id={"tp": peer}, device_id_type=MESH,
        )

    def s1_copy(j):
        cols = span_cols(j)
        return tp_copy(send1.at[:, cols], recv1.at[:, cols], s1_send, s1_recv, j, partner)

    def s2_copy(j):
        cols = span_cols(j)
        return tp_copy(send2.at[:, cols], recv2.at[:, cols], s2_send, s2_recv, j, across)

    def hp_copy(j):
        ref = hid.at[mine, :, span_cols(j)]
        return tp_copy(ref, ref, hp_send, hp_recv, j, partner)

    def hx_copy(j):
        ref = hid.at[mine, :, span_cols(j)]
        return tp_copy(ref, ref, hx_send, hx_recv, j, across)

    def hr_copy(j):
        ref = hid.at[crossed, :, span_cols(j)]
        return tp_copy(ref, ref, hr_send, hr_recv, j, partner)

    for copy in tok_copies:
        copy.wait_recv()

    row = lax.broadcasted_iota(jnp.int32, (LANES, 4 * LANES), 0)
    col = lax.broadcasted_iota(jnp.int32, (LANES, 4 * LANES), 1)
    spread = jnp.where(col % (2 * LANES) == 2 * row + col // (2 * LANES), 1.0, 0.0).astype(BF16)
    ordered = jnp.concatenate([tok_all[b] for b in blocks], axis=0)
    rows = ordered.shape[0]
    stacked = jnp.concatenate(
        [ordered[:, k * LANES:(k + 1) * LANES] for k in range(feat // LANES)], axis=0
    )
    wide = jnp.dot(stacked, spread, preferred_element_type=F32).astype(BF16)
    for k in range(feat // LANES):
        for p in range(4):
            for s in range(2):
                lhs[
                    (2 * p + s) * own_rows:(2 * p + s + 1) * own_rows,
                    2 * k * LANES:2 * (k + 1) * LANES,
                ] = wide[
                    k * rows + p * own_rows:k * rows + (p + 1) * own_rows,
                    2 * s * LANES:2 * (s + 1) * LANES,
                ]

    half = 4 * own_rows

    def store_pair(cols, value):
        keep1[:, cols] = value[:half]
        send1[:, cols] = value[half:].astype(BF16)

    def weight_tile(t):
        return gu.at[t].reshape(2 * feat, LANES)[...]

    def product(j):
        first, count = spans[j]

        def two(i, carry):
            t = first + 2 * i
            gu_copy(t).wait()
            gu_copy(t + 1).wait()
            weight = jnp.concatenate([weight_tile(t), weight_tile(t + 1)], axis=1)
            value = jnp.dot(lhs[...], weight, preferred_element_type=F32)
            store_pair(pl.ds(pl.multiple_of(t * LANES, LANES), 2 * LANES), value)
            return carry

        lax.fori_loop(0, count // 2, two, 0)
        if count % 2:
            t = first + count - 1
            gu_copy(t).wait()
            value = jnp.dot(lhs[...], weight_tile(t), preferred_element_type=F32)
            store_pair(pl.ds(t * LANES, LANES), value)
        s1_copy(j).start()

    def rank_product():
        value = lax.dot_general(
            ordered, ain_pad[...], (((1,), (1,)), ((), ())), preferred_element_type=F32
        )
        blank = jnp.zeros((own_rows, LANES), F32)
        parts = []
        for p in range(4):
            parts += [value[p * own_rows:(p + 1) * own_rows], blank]
        store_pair(pl.ds(hidden, LANES), jnp.concatenate(parts, axis=0))

    def reduce_near(j):
        s1_copy(j).wait_recv()
        cols = span_cols(j)
        value = keep1[:, cols] + recv1[:, cols].astype(F32)
        keep2[:, cols] = value[:2 * own_rows]
        send2[:, cols] = value[2 * own_rows:].astype(BF16)
        s2_copy(j).start()

    def activate(j):
        s2_copy(j).wait_recv()
        first, count = spans[j]
        cols = pl.ds(first * LANES, count * LANES)
        pair = keep2[:, cols] + recv2[:, cols].astype(F32)
        hid[mine, :, cols] = (jax.nn.silu(pair[:own_rows]) * pair[own_rows:]).astype(BF16)
        if j == last:
            cols = pl.ds(hidden, LANES)
            pair = keep2[:own_rows, cols] + recv2[:own_rows, cols].astype(F32)
            hid[mine, :, cols] = pair.astype(BF16)
        hx_copy(j).start()
        hp_copy(j).start()

    def relay(j):
        hx_copy(j).wait_recv()
        hr_copy(j).start()

    def project(j):
        hp_copy(j).wait_recv()
        hr_copy(j).wait_recv()
        down_copy(j).wait()
        first, count = spans[j]
        cols = pl.ds(first * LANES, count * LANES)
        value = jnp.dot(
            hid[:, :, cols].reshape(rows, count * LANES), down[cols, :],
            preferred_element_type=F32,
        )
        if j == 0:
            total[...] = value
        else:
            total[...] += value

    chunk_count = len(spans)
    for j in range(chunk_count):
        product(j)
        if j == 0:
            rank_product()
        else:
            reduce_near(j - 1)
        if j >= 4:
            activate(j - 4)
    reduce_near(last)
    done = max(0, chunk_count - 4)
    for j in range(done, chunk_count):
        activate(j)
        if j >= 2:
            relay(j - 2)
        if j >= 3:
            project(j - 3)
    for j in range(max(0, chunk_count - 2), chunk_count):
        relay(j)
    for j in range(max(0, chunk_count - 3), chunk_count):
        project(j)

    for copy in coef_copies:
        copy.wait_recv()
    rank_mid = hid[:, :, pl.ds(hidden, LANES)].reshape(rows, LANES)
    expert_out = jnp.dot(rank_mid, aout_pad[...], preferred_element_type=F32).astype(BF16)
    all_coef = coef_all[...].reshape(rows, LANES)
    wide_lane = lax.broadcasted_iota(jnp.int32, (rows, LANES), 1)
    column = jnp.sum(jnp.where(wide_lane == me, all_coef, 0.0), axis=1, keepdims=True)
    part = total[...] + column * expert_out.astype(F32)
    total[...] = part
    send_f[...] = part.astype(BF16).reshape(exp_count, own_rows, feat)
    f_copies = [
        exp_copy(send_f.at[(me + d) % exp_count], recv_f.at[d - 1], f_send, f_recv, d)
        for d in range(1, exp_count)
    ]
    for copy in f_copies:
        copy.start()
    result = total[pl.ds(pl.multiple_of(me * own_rows, own_rows), own_rows), :]
    for copy, d in zip(f_copies, range(1, exp_count)):
        copy.wait_recv()
        result = result + recv_f[d - 1].astype(F32)
    out_ref[...] = result.astype(out_ref.dtype)

    for copy in tok_copies + coef_copies + f_copies:
        copy.wait_send()
    for j in range(chunk_count):
        for make in (s1_copy, s2_copy, hp_copy, hx_copy, hr_copy):
            make(j).wait_send()


def fused(tokens, gate_up_weight, down_weight, adapter_in, adapter_out, expert_ids, route_weight):
    exp_count = lax.axis_size("exp")
    own_rows, feat = tokens.shape
    hidden = gate_up_weight.shape[2]
    tiles = hidden // LANES
    chunk_count = len(chunks_of(tiles))
    wide = hidden + LANES
    rows = exp_count * own_rows
    vmem = functools.partial(pltpu.VMEM)
    dma = lambda n: pltpu.SemaphoreType.DMA((n,))
    peers = exp_count - 1
    in_vmem = pl.BlockSpec(memory_space=pltpu.VMEM)
    in_place = pl.BlockSpec(memory_space=pl.ANY)
    return pl.pallas_call(
        functools.partial(kernel, exp_count),
        out_shape=jax.ShapeDtypeStruct((own_rows, feat), BF16),
        in_specs=[in_vmem, in_place, in_place, in_vmem, in_vmem, in_vmem, in_vmem],
        out_specs=in_vmem,
        scratch_shapes=[
            vmem((tiles, feat, 2, LANES), BF16),
            vmem((hidden, feat), BF16),
            vmem((exp_count, own_rows, feat), BF16),
            vmem((exp_count, own_rows, LANES), F32),
            vmem((own_rows, LANES), F32),
            vmem((2 * rows, 2 * feat), BF16),
            vmem((LANES, feat), BF16),
            vmem((LANES, feat), BF16),
            vmem((4 * own_rows, wide), F32),
            vmem((4 * own_rows, wide), BF16),
            vmem((4 * own_rows, wide), BF16),
            vmem((2 * own_rows, wide), F32),
            vmem((2 * own_rows, wide), BF16),
            vmem((2 * own_rows, wide), BF16),
            vmem((4, own_rows, wide), BF16),
            vmem((rows, feat), F32),
            vmem((exp_count, own_rows, feat), BF16),
            vmem((peers, own_rows, feat), BF16),
            dma(tiles), dma(chunk_count),
            dma(peers), dma(peers), dma(peers), dma(peers),
            *[dma(chunk_count) for _ in range(10)],
            dma(peers), dma(peers),
        ],
        compiler_params=pltpu.CompilerParams(
            collective_id=0, has_side_effects=True, vmem_limit_bytes=60 * 2**20
        ),
    )(
        tokens, gate_up_weight, down_weight, jnp.swapaxes(adapter_in, 1, 2), adapter_out,
        expert_ids.T, route_weight.T,
    )


def plain(tokens, gate_up_weight, down_weight, adapter_in, adapter_out, expert_ids, route_weight):
    exp_count = lax.axis_size("exp")
    own_rows, feat_width = tokens.shape
    all_tokens = lax.all_gather(tokens, "exp", axis=0, tiled=True)
    hidden_width = gate_up_weight.shape[2]
    pair_weight = gate_up_weight.reshape(feat_width, 2 * hidden_width)
    pair_share = lax.psum_scatter(
        jnp.dot(all_tokens, pair_weight, preferred_element_type=jnp.float32).astype(jnp.bfloat16),
        "tp",
        scatter_dimension=0,
        tiled=True,
    ).astype(jnp.float32)
    hidden_share = (
        jax.nn.silu(pair_share[:, :hidden_width]) * pair_share[:, hidden_width:]
    ).astype(jnp.bfloat16)
    hidden = lax.all_gather(hidden_share, "tp", axis=0, tiled=True)
    base_out = lax.psum_scatter(
        jnp.dot(hidden, down_weight, preferred_element_type=jnp.float32).astype(jnp.bfloat16),
        "exp",
        scatter_dimension=0,
        tiled=True,
    ).astype(jnp.float32)
    top_count = expert_ids.shape[1]
    expert_count = adapter_in.shape[0] * exp_count
    flat_ids = expert_ids.reshape(own_rows * top_count)
    flat_weight = route_weight.reshape(own_rows * top_count)
    expert_hits = (flat_ids[:, None] == jnp.arange(expert_count, dtype=jnp.int32)[None, :]).astype(
        jnp.int32
    )
    capacity = max(2, 2 * top_count * own_rows // expert_count)
    slot_index = jnp.sum((jnp.cumsum(expert_hits, axis=0) - expert_hits) * expert_hits, axis=1)
    slot_target = flat_ids * capacity + slot_index
    slot_hits = (
        slot_target[:, None] == jnp.arange(expert_count * capacity, dtype=jnp.int32)[None, :]
    )
    combine_matrix = jnp.sum(
        (slot_hits.astype(jnp.float32) * flat_weight[:, None]).reshape(
            own_rows, top_count, expert_count * capacity
        ),
        axis=1,
    )
    dispatch_matrix = slot_hits.T.astype(jnp.bfloat16)
    repeated = jnp.repeat(tokens, top_count, axis=0)
    outgoing = jnp.dot(dispatch_matrix, repeated, preferred_element_type=jnp.float32).astype(
        jnp.bfloat16
    )
    outgoing = outgoing.reshape(expert_count, capacity, feat_width)
    rank_partial = jnp.einsum(
        "scd,dr->scr",
        lax.all_to_all(outgoing, "exp", split_axis=0, concat_axis=0, tiled=True),
        adapter_in[0],
        preferred_element_type=jnp.float32,
    )
    rank_mid = lax.psum(rank_partial, "tp").astype(jnp.bfloat16)
    expert_out = jnp.einsum(
        "scr,rd->scd", rank_mid, adapter_out[0], preferred_element_type=jnp.float32
    ).astype(jnp.bfloat16)
    returned = lax.all_to_all(expert_out, "exp", split_axis=0, concat_axis=0, tiled=True)
    adapter_sum = jnp.dot(
        combine_matrix,
        returned.reshape(expert_count * capacity, feat_width).astype(jnp.float32),
        precision=lax.Precision.HIGHEST,
        preferred_element_type=jnp.float32,
    )
    return (base_out + adapter_sum).astype(jnp.bfloat16)


def local(tokens, gate_up_weight, *rest):
    own_rows, feat = tokens.shape
    fits = (
        lax.axis_size("tp") == 4
        and lax.axis_size("exp") == 4
        and rest[1].shape[0] == 1
        and rest[1].shape[2] <= LANES
        and own_rows % 16 == 0
        and feat % LANES == 0
        and gate_up_weight.shape[2] % LANES == 0
    )
    return (fused if fits else plain)(tokens, gate_up_weight, *rest)


def solution(mesh):
    in_specs = (
        P(("grp", "exp"), "tp"),
        P("tp", None, "exp"),
        P("exp", "tp"),
        P("exp", "tp", None),
        P("exp", None, "tp"),
        P(("grp", "exp"), None),
        P(("grp", "exp"), None),
    )
    out_specs = P(("grp", "exp"), "tp")
    return jax.shard_map(local, mesh=mesh, in_specs=in_specs, out_specs=out_specs, check_vma=False)
```

```python
import functools
import jax
import jax.numpy as jnp
from jax import lax
from jax.experimental import pallas as pl
from jax.experimental.pallas import tpu as pltpu
from jax.sharding import PartitionSpec as P

LANES = 128
CHUNK_TILES = 8
STEP_TILES = 4
MESH = pl.DeviceIdType.MESH
BF16, F32 = jnp.bfloat16, jnp.float32


def chunks_of(tiles):
    spans, first = [], 0
    while first < tiles:
        count = min(CHUNK_TILES, tiles - first)
        spans.append((first, count))
        first += count
    return spans


def kernel(
    exp_count, tok_ref, gu_ref, down_ref, ain_ref, aout_ref, ids_ref, weight_ref, out_ref,
    gu, down, tok_all, coef_all, coef_own, lhs, ain_pad, aout_pad,
    keep1, send1, recv1, keep2, send2, recv2, hid, total, send_f, recv_f,
    gu_sem, down_sem, tok_send, tok_recv, coef_send, coef_recv,
    s1_send, s1_recv, s2_send, s2_recv, hp_send, hp_recv, hx_send, hx_recv, hr_send, hr_recv,
    f_send, f_recv,
):
    me = lax.axis_index("exp")
    tp = lax.axis_index("tp")
    own_rows, feat = tok_ref.shape
    hidden = gu_ref.shape[2]
    rank = ain_ref.shape[1]
    tiles = hidden // LANES
    spans = chunks_of(tiles)
    last = len(spans) - 1
    core, side = tp % 2, tp // 2
    partner = side * 2 + (1 - core)
    across = (1 - side) * 2 + core
    blocks = [
        core * 2 + side,
        core * 2 + (1 - side),
        (1 - core) * 2 + side,
        (1 - core) * 2 + (1 - side),
    ]
    mine, crossed = blocks[0], blocks[1]

    gu_flat = gu_ref.reshape(2 * feat, hidden)

    def gu_copy(t):
        cols = pl.ds(pl.multiple_of(t * LANES, LANES), LANES)
        return pltpu.make_async_copy(gu_flat.at[:, cols], gu.at[t], gu_sem.at[t])

    def down_copy(j):
        first, count = spans[j]
        rows = pl.ds(first * LANES, count * LANES)
        return pltpu.make_async_copy(down_ref.at[rows], down.at[rows], down_sem.at[j])

    def start_gu(t, carry):
        gu_copy(t).start()
        return carry

    lax.fori_loop(0, tiles, start_gu, 0)
    for j in range(len(spans)):
        down_copy(j).start()

    barrier = pltpu.get_barrier_semaphore()
    for d in range(1, exp_count):
        pl.semaphore_signal(
            barrier, inc=1, device_id={"exp": (me + d) % exp_count}, device_id_type=MESH
        )
    for peer in (partner, across):
        pl.semaphore_signal(barrier, inc=1, device_id={"tp": peer}, device_id_type=MESH)

    lane = lax.broadcasted_iota(jnp.int32, (own_rows, LANES), 1)
    diagonal = lax.broadcasted_iota(
        jnp.int32, (own_rows, own_rows), 0
    ) == lax.broadcasted_iota(jnp.int32, (own_rows, own_rows), 1)

    def column_of(line):
        return jnp.sum(jnp.where(diagonal, line, 0.0), axis=1, keepdims=True)

    coef = jnp.zeros((own_rows, LANES), F32)
    for k in range(ids_ref.shape[0]):
        named = column_of(ids_ref[k:k + 1, :].astype(F32)).astype(jnp.int32)
        coef = coef + jnp.where(lane == named, column_of(weight_ref[k:k + 1, :]), 0.0)
    coef_own[...] = coef
    coef_all[me] = coef
    tok_all[me] = tok_ref[...]
    ain_pad[...] = jnp.zeros_like(ain_pad)
    ain_pad[:rank, :] = ain_ref[0]
    aout_pad[...] = jnp.zeros_like(aout_pad)
    aout_pad[:rank, :] = aout_ref[0]

    pl.semaphore_wait(barrier, exp_count + 1)

    def exp_copy(src, dst, send, recv, d):
        return pltpu.make_async_remote_copy(
            src_ref=src, dst_ref=dst, send_sem=send.at[d - 1], recv_sem=recv.at[d - 1],
            device_id={"exp": (me + d) % exp_count}, device_id_type=MESH,
        )

    tok_copies = [
        exp_copy(tok_ref, tok_all.at[me], tok_send, tok_recv, d) for d in range(1, exp_count)
    ]
    coef_copies = [
        exp_copy(coef_own, coef_all.at[me], coef_send, coef_recv, d) for d in range(1, exp_count)
    ]
    for copy in tok_copies + coef_copies:
        copy.start()

    def span_cols(j):
        first, count = spans[j]
        if j == 0:
            return pl.ds(0, (count + 1) * LANES)
        return pl.ds((first + 1) * LANES, count * LANES)

    def tp_copy(src, dst, send, recv, j, peer):
        return pltpu.make_async_remote_copy(
            src_ref=src, dst_ref=dst, send_sem=send.at[j], recv_sem=recv.at[j],
            device_id={"tp": peer}, device_id_type=MESH,
        )

    def s1_copy(j):
        cols = span_cols(j)
        return tp_copy(send1.at[:, cols], recv1.at[:, cols], s1_send, s1_recv, j, partner)

    def s2_copy(j):
        cols = span_cols(j)
        return tp_copy(send2.at[:, cols], recv2.at[:, cols], s2_send, s2_recv, j, across)

    def hp_copy(j):
        ref = hid.at[mine, :, span_cols(j)]
        return tp_copy(ref, ref, hp_send, hp_recv, j, partner)

    def hx_copy(j):
        ref = hid.at[mine, :, span_cols(j)]
        return tp_copy(ref, ref, hx_send, hx_recv, j, across)

    def hr_copy(j):
        ref = hid.at[crossed, :, span_cols(j)]
        return tp_copy(ref, ref, hr_send, hr_recv, j, partner)

    for copy in tok_copies:
        copy.wait_recv()

    row = lax.broadcasted_iota(jnp.int32, (LANES, 4 * LANES), 0)
    col = lax.broadcasted_iota(jnp.int32, (LANES, 4 * LANES), 1)
    spread = jnp.where(col % (2 * LANES) == 2 * row + col // (2 * LANES), 1.0, 0.0).astype(BF16)
    ordered = jnp.concatenate([tok_all[b] for b in blocks], axis=0)
    rows = ordered.shape[0]
    stacked = jnp.concatenate(
        [ordered[:, k * LANES:(k + 1) * LANES] for k in range(feat // LANES)], axis=0
    )
    wide = jnp.dot(stacked, spread, preferred_element_type=F32).astype(BF16)
    for k in range(feat // LANES):
        for p in range(4):
            for s in range(2):
                lhs[
                    (2 * p + s) * own_rows:(2 * p + s + 1) * own_rows,
                    2 * k * LANES:2 * (k + 1) * LANES,
                ] = wide[
                    k * rows + p * own_rows:k * rows + (p + 1) * own_rows,
                    2 * s * LANES:2 * (s + 1) * LANES,
                ]

    half = 4 * own_rows

    def store_pair(cols, value):
        keep1[:, cols] = value[:half]
        send1[:, cols] = value[half:].astype(BF16)

    def product(j):
        first, count = spans[j]

        def several(t, width):
            for i in range(width):
                gu_copy(t + i).wait()
            weight = jnp.concatenate([gu[t + i] for i in range(width)], axis=1)
            value = jnp.dot(lhs[...], weight, preferred_element_type=F32)
            store_pair(pl.ds(pl.multiple_of((t + 1) * LANES, LANES), width * LANES), value)

        def step(i, carry):
            several(first + STEP_TILES * i, STEP_TILES)
            return carry

        lax.fori_loop(0, count // STEP_TILES, step, 0)
        if count % STEP_TILES:
            several(first + count - count % STEP_TILES, count % STEP_TILES)
        s1_copy(j).start()

    def rank_product():
        value = lax.dot_general(
            ordered, ain_pad[...], (((1,), (1,)), ((), ())), preferred_element_type=F32
        )
        blank = jnp.zeros((own_rows, LANES), F32)
        parts = []
        for p in range(4):
            parts += [value[p * own_rows:(p + 1) * own_rows], blank]
        store_pair(pl.ds(0, LANES), jnp.concatenate(parts, axis=0))

    def reduce_near(j):
        s1_copy(j).wait_recv()
        cols = span_cols(j)
        value = keep1[:, cols] + recv1[:, cols].astype(F32)
        keep2[:, cols] = value[:2 * own_rows]
        send2[:, cols] = value[2 * own_rows:].astype(BF16)
        s2_copy(j).start()

    def activate(j):
        s2_copy(j).wait_recv()
        first, count = spans[j]
        cols = pl.ds((first + 1) * LANES, count * LANES)
        pair = keep2[:, cols] + recv2[:, cols].astype(F32)
        hid[mine, :, cols] = (jax.nn.silu(pair[:own_rows]) * pair[own_rows:]).astype(BF16)
        if j == 0:
            cols = pl.ds(0, LANES)
            pair = keep2[:own_rows, cols] + recv2[:own_rows, cols].astype(F32)
            hid[mine, :, cols] = pair.astype(BF16)
        hx_copy(j).start()
        hp_copy(j).start()

    def relay(j):
        hx_copy(j).wait_recv()
        hr_copy(j).start()

    def adapter_part():
        for copy in coef_copies:
            copy.wait_recv()
        rank_mid = hid[:, :, pl.ds(0, LANES)].reshape(rows, LANES)
        expert_out = jnp.dot(rank_mid, aout_pad[...], preferred_element_type=F32).astype(BF16)
        all_coef = coef_all[...].reshape(rows, LANES)
        wide_lane = lax.broadcasted_iota(jnp.int32, (rows, LANES), 1)
        column = jnp.sum(jnp.where(wide_lane == me, all_coef, 0.0), axis=1, keepdims=True)
        return column * expert_out.astype(F32)

    def project(j):
        hp_copy(j).wait_recv()
        hr_copy(j).wait_recv()
        down_copy(j).wait()
        first, count = spans[j]
        cols = pl.ds((first + 1) * LANES, count * LANES)
        value = jnp.dot(
            hid[:, :, cols].reshape(rows, count * LANES),
            down[pl.ds(first * LANES, count * LANES), :],
            preferred_element_type=F32,
        )
        if j == 0:
            total[...] = value + adapter_part()
        else:
            total[...] += value

    chunk_count = len(spans)
    for j in range(chunk_count):
        if j == 0:
            rank_product()
        product(j)
        if j > 0:
            reduce_near(j - 1)
        if j >= 4:
            activate(j - 4)
    reduce_near(last)
    done = max(0, chunk_count - 4)
    for j in range(done, chunk_count):
        activate(j)
        if j >= 2:
            relay(j - 2)
        if j >= 3:
            project(j - 3)
    for j in range(max(0, chunk_count - 2), chunk_count):
        relay(j)
    for j in range(max(0, chunk_count - 3), chunk_count):
        project(j)

    part = total[...]
    send_f[...] = part.astype(BF16).reshape(exp_count, own_rows, feat)
    f_copies = [
        exp_copy(send_f.at[(me + d) % exp_count], recv_f.at[d - 1], f_send, f_recv, d)
        for d in range(1, exp_count)
    ]
    for copy in f_copies:
        copy.start()
    result = total[pl.ds(pl.multiple_of(me * own_rows, own_rows), own_rows), :]
    for copy, d in zip(f_copies, range(1, exp_count)):
        copy.wait_recv()
        result = result + recv_f[d - 1].astype(F32)
    out_ref[...] = result.astype(out_ref.dtype)

    for copy in tok_copies + coef_copies + f_copies:
        copy.wait_send()
    for j in range(chunk_count):
        for make in (s1_copy, s2_copy, hp_copy, hx_copy, hr_copy):
            make(j).wait_send()


def fused(tokens, gate_up_weight, down_weight, adapter_in, adapter_out, expert_ids, route_weight):
    exp_count = lax.axis_size("exp")
    own_rows, feat = tokens.shape
    hidden = gate_up_weight.shape[2]
    tiles = hidden // LANES
    chunk_count = len(chunks_of(tiles))
    wide = hidden + LANES
    rows = exp_count * own_rows
    vmem = functools.partial(pltpu.VMEM)
    dma = lambda n: pltpu.SemaphoreType.DMA((n,))
    peers = exp_count - 1
    in_vmem = pl.BlockSpec(memory_space=pltpu.VMEM)
    in_place = pl.BlockSpec(memory_space=pl.ANY)
    return pl.pallas_call(
        functools.partial(kernel, exp_count),
        out_shape=jax.ShapeDtypeStruct((own_rows, feat), BF16),
        in_specs=[in_vmem, in_place, in_place, in_vmem, in_vmem, in_vmem, in_vmem],
        out_specs=in_vmem,
        scratch_shapes=[
            vmem((tiles, 2 * feat, LANES), BF16),
            vmem((hidden, feat), BF16),
            vmem((exp_count, own_rows, feat), BF16),
            vmem((exp_count, own_rows, LANES), F32),
            vmem((own_rows, LANES), F32),
            vmem((2 * rows, 2 * feat), BF16),
            vmem((LANES, feat), BF16),
            vmem((LANES, feat), BF16),
            vmem((4 * own_rows, wide), F32),
            vmem((4 * own_rows, wide), BF16),
            vmem((4 * own_rows, wide), BF16),
            vmem((2 * own_rows, wide), F32),
            vmem((2 * own_rows, wide), BF16),
            vmem((2 * own_rows, wide), BF16),
            vmem((4, own_rows, wide), BF16),
            vmem((rows, feat), F32),
            vmem((exp_count, own_rows, feat), BF16),
            vmem((peers, own_rows, feat), BF16),
            dma(tiles), dma(chunk_count),
            dma(peers), dma(peers), dma(peers), dma(peers),
            *[dma(chunk_count) for _ in range(10)],
            dma(peers), dma(peers),
        ],
        compiler_params=pltpu.CompilerParams(
            collective_id=0, has_side_effects=True, vmem_limit_bytes=60 * 2**20
        ),
    )(
        tokens, gate_up_weight, down_weight, jnp.swapaxes(adapter_in, 1, 2), adapter_out,
        expert_ids.T, route_weight.T,
    )


def plain(tokens, gate_up_weight, down_weight, adapter_in, adapter_out, expert_ids, route_weight):
    exp_count = lax.axis_size("exp")
    own_rows, feat_width = tokens.shape
    all_tokens = lax.all_gather(tokens, "exp", axis=0, tiled=True)
    hidden_width = gate_up_weight.shape[2]
    pair_weight = gate_up_weight.reshape(feat_width, 2 * hidden_width)
    pair_share = lax.psum_scatter(
        jnp.dot(all_tokens, pair_weight, preferred_element_type=jnp.float32).astype(jnp.bfloat16),
        "tp",
        scatter_dimension=0,
        tiled=True,
    ).astype(jnp.float32)
    hidden_share = (
        jax.nn.silu(pair_share[:, :hidden_width]) * pair_share[:, hidden_width:]
    ).astype(jnp.bfloat16)
    hidden = lax.all_gather(hidden_share, "tp", axis=0, tiled=True)
    base_out = lax.psum_scatter(
        jnp.dot(hidden, down_weight, preferred_element_type=jnp.float32).astype(jnp.bfloat16),
        "exp",
        scatter_dimension=0,
        tiled=True,
    ).astype(jnp.float32)
    top_count = expert_ids.shape[1]
    expert_count = adapter_in.shape[0] * exp_count
    flat_ids = expert_ids.reshape(own_rows * top_count)
    flat_weight = route_weight.reshape(own_rows * top_count)
    expert_hits = (flat_ids[:, None] == jnp.arange(expert_count, dtype=jnp.int32)[None, :]).astype(
        jnp.int32
    )
    capacity = max(2, 2 * top_count * own_rows // expert_count)
    slot_index = jnp.sum((jnp.cumsum(expert_hits, axis=0) - expert_hits) * expert_hits, axis=1)
    slot_target = flat_ids * capacity + slot_index
    slot_hits = (
        slot_target[:, None] == jnp.arange(expert_count * capacity, dtype=jnp.int32)[None, :]
    )
    combine_matrix = jnp.sum(
        (slot_hits.astype(jnp.float32) * flat_weight[:, None]).reshape(
            own_rows, top_count, expert_count * capacity
        ),
        axis=1,
    )
    dispatch_matrix = slot_hits.T.astype(jnp.bfloat16)
    repeated = jnp.repeat(tokens, top_count, axis=0)
    outgoing = jnp.dot(dispatch_matrix, repeated, preferred_element_type=jnp.float32).astype(
        jnp.bfloat16
    )
    outgoing = outgoing.reshape(expert_count, capacity, feat_width)
    rank_partial = jnp.einsum(
        "scd,dr->scr",
        lax.all_to_all(outgoing, "exp", split_axis=0, concat_axis=0, tiled=True),
        adapter_in[0],
        preferred_element_type=jnp.float32,
    )
    rank_mid = lax.psum(rank_partial, "tp").astype(jnp.bfloat16)
    expert_out = jnp.einsum(
        "scr,rd->scd", rank_mid, adapter_out[0], preferred_element_type=jnp.float32
    ).astype(jnp.bfloat16)
    returned = lax.all_to_all(expert_out, "exp", split_axis=0, concat_axis=0, tiled=True)
    adapter_sum = jnp.dot(
        combine_matrix,
        returned.reshape(expert_count * capacity, feat_width).astype(jnp.float32),
        precision=lax.Precision.HIGHEST,
        preferred_element_type=jnp.float32,
    )
    return (base_out + adapter_sum).astype(jnp.bfloat16)


def local(tokens, gate_up_weight, *rest):
    own_rows, feat = tokens.shape
    fits = (
        lax.axis_size("tp") == 4
        and lax.axis_size("exp") == 4
        and rest[1].shape[0] == 1
        and rest[1].shape[2] <= LANES
        and own_rows % 16 == 0
        and feat % LANES == 0
        and gate_up_weight.shape[2] % LANES == 0
    )
    return (fused if fits else plain)(tokens, gate_up_weight, *rest)


def solution(mesh):
    in_specs = (
        P(("grp", "exp"), "tp"),
        P("tp", None, "exp"),
        P("exp", "tp"),
        P("exp", "tp", None),
        P("exp", None, "tp"),
        P(("grp", "exp"), None),
        P(("grp", "exp"), None),
    )
    out_specs = P(("grp", "exp"), "tp")
    return jax.shard_map(local, mesh=mesh, in_specs=in_specs, out_specs=out_specs, check_vma=False)
```

```python
import functools
import jax
import jax.numpy as jnp
from jax import lax
from jax.experimental import pallas as pl
from jax.experimental.pallas import tpu as pltpu
from jax.sharding import PartitionSpec as P

LANES = 128
CHUNK_TILES = 6
STEP_TILES = 6
RELAY_LAG = 6
MESH = pl.DeviceIdType.MESH
BF16, F32 = jnp.bfloat16, jnp.float32


def chunks_of(tiles):
    spans, first = [], 0
    while first < tiles:
        count = min(CHUNK_TILES, tiles - first)
        spans.append((first, count))
        first += count
    return spans


def kernel(
    exp_count, tok_ref, gu_ref, down_ref, ain_ref, aout_ref, ids_ref, weight_ref, out_ref,
    gu, down, tok_all, coef_all, coef_own, lhs, ain_pad, aout_pad,
    keep1, send1, recv1, keep2, send2, recv2, hid, total, send_f, recv_f,
    gu_sem, down_sem, tok_send, tok_recv, coef_send, coef_recv,
    s1_send, s1_recv, s2_send, s2_recv, hp_send, hp_recv, hx_send, hx_recv, hr_send, hr_recv,
    f_send, f_recv,
):
    me = lax.axis_index("exp")
    tp = lax.axis_index("tp")
    own_rows, feat = tok_ref.shape
    hidden = gu_ref.shape[2]
    rank = ain_ref.shape[1]
    tiles = hidden // LANES
    spans = chunks_of(tiles)
    core, side = tp % 2, tp // 2
    partner = side * 2 + (1 - core)
    across = (1 - side) * 2 + core
    blocks = [
        core * 2 + side,
        core * 2 + (1 - side),
        (1 - core) * 2 + side,
        (1 - core) * 2 + (1 - side),
    ]
    mine, crossed = blocks[0], blocks[1]

    gu_flat = gu_ref.reshape(2 * feat, hidden)

    def gu_copy(t):
        cols = pl.ds(pl.multiple_of(t * LANES, LANES), LANES)
        return pltpu.make_async_copy(gu_flat.at[:, cols], gu.at[t], gu_sem.at[t])

    def down_copy(j):
        first, count = spans[j]
        rows = pl.ds(first * LANES, count * LANES)
        return pltpu.make_async_copy(down_ref.at[rows], down.at[rows], down_sem.at[j])

    def start_gu(t, carry):
        gu_copy(t).start()
        return carry

    lax.fori_loop(0, tiles, start_gu, 0)
    for j in range(len(spans)):
        down_copy(j).start()

    barrier = pltpu.get_barrier_semaphore()
    for d in range(1, exp_count):
        pl.semaphore_signal(
            barrier, inc=1, device_id={"exp": (me + d) % exp_count}, device_id_type=MESH
        )
    for peer in (partner, across):
        pl.semaphore_signal(barrier, inc=1, device_id={"tp": peer}, device_id_type=MESH)

    lane = lax.broadcasted_iota(jnp.int32, (own_rows, LANES), 1)
    diagonal = lax.broadcasted_iota(
        jnp.int32, (own_rows, own_rows), 0
    ) == lax.broadcasted_iota(jnp.int32, (own_rows, own_rows), 1)

    def column_of(line):
        return jnp.sum(jnp.where(diagonal, line, 0.0), axis=1, keepdims=True)

    coef = jnp.zeros((own_rows, LANES), F32)
    for k in range(ids_ref.shape[0]):
        named = column_of(ids_ref[k:k + 1, :].astype(F32)).astype(jnp.int32)
        coef = coef + jnp.where(lane == named, column_of(weight_ref[k:k + 1, :]), 0.0)
    coef_own[...] = coef
    coef_all[me] = coef
    tok_all[me] = tok_ref[...]
    ain_pad[...] = jnp.zeros_like(ain_pad)
    ain_pad[:rank, :] = ain_ref[0]
    aout_pad[...] = jnp.zeros_like(aout_pad)
    aout_pad[:rank, :] = aout_ref[0]

    pl.semaphore_wait(barrier, exp_count + 1)

    def exp_copy(src, dst, send, recv, d):
        return pltpu.make_async_remote_copy(
            src_ref=src, dst_ref=dst, send_sem=send.at[d - 1], recv_sem=recv.at[d - 1],
            device_id={"exp": (me + d) % exp_count}, device_id_type=MESH,
        )

    tok_copies = [
        exp_copy(tok_ref, tok_all.at[me], tok_send, tok_recv, d) for d in range(1, exp_count)
    ]
    coef_copies = [
        exp_copy(coef_own, coef_all.at[me], coef_send, coef_recv, d) for d in range(1, exp_count)
    ]
    for copy in tok_copies + coef_copies:
        copy.start()

    def span_cols(j):
        first, count = spans[j]
        if j == 0:
            return pl.ds(0, (count + 1) * LANES)
        return pl.ds((first + 1) * LANES, count * LANES)

    def tp_copy(src, dst, send, recv, j, peer):
        return pltpu.make_async_remote_copy(
            src_ref=src, dst_ref=dst, send_sem=send.at[j], recv_sem=recv.at[j],
            device_id={"tp": peer}, device_id_type=MESH,
        )

    def s1_copy(j):
        cols = span_cols(j)
        return tp_copy(send1.at[:, cols], recv1.at[:, cols], s1_send, s1_recv, j, partner)

    def s2_copy(j):
        cols = span_cols(j)
        return tp_copy(send2.at[:, cols], recv2.at[:, cols], s2_send, s2_recv, j, across)

    def hp_copy(j):
        ref = hid.at[mine, :, span_cols(j)]
        return tp_copy(ref, ref, hp_send, hp_recv, j, partner)

    def hx_copy(j):
        ref = hid.at[mine, :, span_cols(j)]
        return tp_copy(ref, ref, hx_send, hx_recv, j, across)

    def hr_copy(j):
        ref = hid.at[crossed, :, span_cols(j)]
        return tp_copy(ref, ref, hr_send, hr_recv, j, partner)

    for copy in tok_copies:
        copy.wait_recv()

    row = lax.broadcasted_iota(jnp.int32, (LANES, 4 * LANES), 0)
    col = lax.broadcasted_iota(jnp.int32, (LANES, 4 * LANES), 1)
    spread = jnp.where(col % (2 * LANES) == 2 * row + col // (2 * LANES), 1.0, 0.0).astype(BF16)
    ordered = jnp.concatenate([tok_all[b] for b in blocks], axis=0)
    rows = ordered.shape[0]
    stacked = jnp.concatenate(
        [ordered[:, k * LANES:(k + 1) * LANES] for k in range(feat // LANES)], axis=0
    )
    wide = jnp.dot(stacked, spread, preferred_element_type=F32).astype(BF16)
    for k in range(feat // LANES):
        for p in range(4):
            for s in range(2):
                lhs[
                    (2 * p + s) * own_rows:(2 * p + s + 1) * own_rows,
                    2 * k * LANES:2 * (k + 1) * LANES,
                ] = wide[
                    k * rows + p * own_rows:k * rows + (p + 1) * own_rows,
                    2 * s * LANES:2 * (s + 1) * LANES,
                ]

    half = 4 * own_rows

    def store_pair(cols, value):
        keep1[:, cols] = value[:half]
        send1[:, cols] = value[half:].astype(BF16)

    def product(j):
        first, count = spans[j]

        def several(t, width):
            for i in range(width):
                gu_copy(t + i).wait()
            weight = jnp.concatenate([gu[t + i] for i in range(width)], axis=1)
            value = jnp.dot(lhs[...], weight, preferred_element_type=F32)
            store_pair(pl.ds(pl.multiple_of((t + 1) * LANES, LANES), width * LANES), value)

        def step(i, carry):
            several(first + STEP_TILES * i, STEP_TILES)
            return carry

        lax.fori_loop(0, count // STEP_TILES, step, 0)
        if count % STEP_TILES:
            several(first + count - count % STEP_TILES, count % STEP_TILES)
        s1_copy(j).start()

    def rank_product():
        value = lax.dot_general(
            ordered, ain_pad[...], (((1,), (1,)), ((), ())), preferred_element_type=F32
        )
        blank = jnp.zeros((own_rows, LANES), F32)
        parts = []
        for p in range(4):
            parts += [value[p * own_rows:(p + 1) * own_rows], blank]
        store_pair(pl.ds(0, LANES), jnp.concatenate(parts, axis=0))

    def reduce_near(j):
        s1_copy(j).wait_recv()
        cols = span_cols(j)
        value = keep1[:, cols] + recv1[:, cols].astype(F32)
        keep2[:, cols] = value[:2 * own_rows]
        send2[:, cols] = value[2 * own_rows:].astype(BF16)
        s2_copy(j).start()

    def activate(j):
        s2_copy(j).wait_recv()
        first, count = spans[j]
        cols = pl.ds((first + 1) * LANES, count * LANES)
        pair = keep2[:, cols] + recv2[:, cols].astype(F32)
        hid[mine, :, cols] = (jax.nn.silu(pair[:own_rows]) * pair[own_rows:]).astype(BF16)
        if j == 0:
            cols = pl.ds(0, LANES)
            pair = keep2[:own_rows, cols] + recv2[:own_rows, cols].astype(F32)
            hid[mine, :, cols] = pair.astype(BF16)
        hx_copy(j).start()
        hp_copy(j).start()

    def relay(j):
        hx_copy(j).wait_recv()
        hr_copy(j).start()

    def adapter_part():
        for copy in coef_copies:
            copy.wait_recv()
        rank_mid = hid[:, :, pl.ds(0, LANES)].reshape(rows, LANES)
        expert_out = jnp.dot(rank_mid, aout_pad[...], preferred_element_type=F32).astype(BF16)
        all_coef = coef_all[...].reshape(rows, LANES)
        wide_lane = lax.broadcasted_iota(jnp.int32, (rows, LANES), 1)
        column = jnp.sum(jnp.where(wide_lane == me, all_coef, 0.0), axis=1, keepdims=True)
        return column * expert_out.astype(F32)

    def project(j):
        hp_copy(j).wait_recv()
        hr_copy(j).wait_recv()
        down_copy(j).wait()
        first, count = spans[j]
        cols = pl.ds((first + 1) * LANES, count * LANES)
        value = jnp.dot(
            hid[:, :, cols].reshape(rows, count * LANES),
            down[pl.ds(first * LANES, count * LANES), :],
            preferred_element_type=F32,
        )
        if j == 0:
            total[...] = value + adapter_part()
        else:
            total[...] += value

    chunk_count = len(spans)
    stages = (
        (product, 0), (reduce_near, 1), (activate, 4), (relay, RELAY_LAG), (project, RELAY_LAG + 1),
    )
    rank_product()
    for step in range(chunk_count + RELAY_LAG + 1):
        for stage, lag in stages:
            if 0 <= step - lag < chunk_count:
                stage(step - lag)

    part = total[...]
    send_f[...] = part.astype(BF16).reshape(exp_count, own_rows, feat)
    f_copies = [
        exp_copy(send_f.at[(me + d) % exp_count], recv_f.at[d - 1], f_send, f_recv, d)
        for d in range(1, exp_count)
    ]
    for copy in f_copies:
        copy.start()
    result = total[pl.ds(pl.multiple_of(me * own_rows, own_rows), own_rows), :]
    for copy, d in zip(f_copies, range(1, exp_count)):
        copy.wait_recv()
        result = result + recv_f[d - 1].astype(F32)
    out_ref[...] = result.astype(out_ref.dtype)

    for copy in tok_copies + coef_copies + f_copies:
        copy.wait_send()
    for j in range(chunk_count):
        for make in (s1_copy, s2_copy, hp_copy, hx_copy, hr_copy):
            make(j).wait_send()


def fused(tokens, gate_up_weight, down_weight, adapter_in, adapter_out, expert_ids, route_weight):
    exp_count = lax.axis_size("exp")
    own_rows, feat = tokens.shape
    hidden = gate_up_weight.shape[2]
    tiles = hidden // LANES
    chunk_count = len(chunks_of(tiles))
    wide = hidden + LANES
    rows = exp_count * own_rows
    vmem = functools.partial(pltpu.VMEM)
    dma = lambda n: pltpu.SemaphoreType.DMA((n,))
    peers = exp_count - 1
    in_vmem = pl.BlockSpec(memory_space=pltpu.VMEM)
    in_place = pl.BlockSpec(memory_space=pl.ANY)
    return pl.pallas_call(
        functools.partial(kernel, exp_count),
        out_shape=jax.ShapeDtypeStruct((own_rows, feat), BF16),
        in_specs=[in_vmem, in_place, in_place, in_vmem, in_vmem, in_vmem, in_vmem],
        out_specs=in_vmem,
        scratch_shapes=[
            vmem((tiles, 2 * feat, LANES), BF16),
            vmem((hidden, feat), BF16),
            vmem((exp_count, own_rows, feat), BF16),
            vmem((exp_count, own_rows, LANES), F32),
            vmem((own_rows, LANES), F32),
            vmem((2 * rows, 2 * feat), BF16),
            vmem((LANES, feat), BF16),
            vmem((LANES, feat), BF16),
            vmem((4 * own_rows, wide), F32),
            vmem((4 * own_rows, wide), BF16),
            vmem((4 * own_rows, wide), BF16),
            vmem((2 * own_rows, wide), F32),
            vmem((2 * own_rows, wide), BF16),
            vmem((2 * own_rows, wide), BF16),
            vmem((4, own_rows, wide), BF16),
            vmem((rows, feat), F32),
            vmem((exp_count, own_rows, feat), BF16),
            vmem((peers, own_rows, feat), BF16),
            dma(tiles), dma(chunk_count),
            dma(peers), dma(peers), dma(peers), dma(peers),
            *[dma(chunk_count) for _ in range(10)],
            dma(peers), dma(peers),
        ],
        compiler_params=pltpu.CompilerParams(
            collective_id=0, has_side_effects=True, vmem_limit_bytes=60 * 2**20
        ),
    )(
        tokens, gate_up_weight, down_weight, jnp.swapaxes(adapter_in, 1, 2), adapter_out,
        expert_ids.T, route_weight.T,
    )


def plain(tokens, gate_up_weight, down_weight, adapter_in, adapter_out, expert_ids, route_weight):
    exp_count = lax.axis_size("exp")
    own_rows, feat_width = tokens.shape
    all_tokens = lax.all_gather(tokens, "exp", axis=0, tiled=True)
    hidden_width = gate_up_weight.shape[2]
    pair_weight = gate_up_weight.reshape(feat_width, 2 * hidden_width)
    pair_share = lax.psum_scatter(
        jnp.dot(all_tokens, pair_weight, preferred_element_type=jnp.float32).astype(jnp.bfloat16),
        "tp",
        scatter_dimension=0,
        tiled=True,
    ).astype(jnp.float32)
    hidden_share = (
        jax.nn.silu(pair_share[:, :hidden_width]) * pair_share[:, hidden_width:]
    ).astype(jnp.bfloat16)
    hidden = lax.all_gather(hidden_share, "tp", axis=0, tiled=True)
    base_out = lax.psum_scatter(
        jnp.dot(hidden, down_weight, preferred_element_type=jnp.float32).astype(jnp.bfloat16),
        "exp",
        scatter_dimension=0,
        tiled=True,
    ).astype(jnp.float32)
    top_count = expert_ids.shape[1]
    expert_count = adapter_in.shape[0] * exp_count
    flat_ids = expert_ids.reshape(own_rows * top_count)
    flat_weight = route_weight.reshape(own_rows * top_count)
    expert_hits = (flat_ids[:, None] == jnp.arange(expert_count, dtype=jnp.int32)[None, :]).astype(
        jnp.int32
    )
    capacity = max(2, 2 * top_count * own_rows // expert_count)
    slot_index = jnp.sum((jnp.cumsum(expert_hits, axis=0) - expert_hits) * expert_hits, axis=1)
    slot_target = flat_ids * capacity + slot_index
    slot_hits = (
        slot_target[:, None] == jnp.arange(expert_count * capacity, dtype=jnp.int32)[None, :]
    )
    combine_matrix = jnp.sum(
        (slot_hits.astype(jnp.float32) * flat_weight[:, None]).reshape(
            own_rows, top_count, expert_count * capacity
        ),
        axis=1,
    )
    dispatch_matrix = slot_hits.T.astype(jnp.bfloat16)
    repeated = jnp.repeat(tokens, top_count, axis=0)
    outgoing = jnp.dot(dispatch_matrix, repeated, preferred_element_type=jnp.float32).astype(
        jnp.bfloat16
    )
    outgoing = outgoing.reshape(expert_count, capacity, feat_width)
    rank_partial = jnp.einsum(
        "scd,dr->scr",
        lax.all_to_all(outgoing, "exp", split_axis=0, concat_axis=0, tiled=True),
        adapter_in[0],
        preferred_element_type=jnp.float32,
    )
    rank_mid = lax.psum(rank_partial, "tp").astype(jnp.bfloat16)
    expert_out = jnp.einsum(
        "scr,rd->scd", rank_mid, adapter_out[0], preferred_element_type=jnp.float32
    ).astype(jnp.bfloat16)
    returned = lax.all_to_all(expert_out, "exp", split_axis=0, concat_axis=0, tiled=True)
    adapter_sum = jnp.dot(
        combine_matrix,
        returned.reshape(expert_count * capacity, feat_width).astype(jnp.float32),
        precision=lax.Precision.HIGHEST,
        preferred_element_type=jnp.float32,
    )
    return (base_out + adapter_sum).astype(jnp.bfloat16)


def local(tokens, gate_up_weight, *rest):
    own_rows, feat = tokens.shape
    fits = (
        lax.axis_size("tp") == 4
        and lax.axis_size("exp") == 4
        and rest[1].shape[0] == 1
        and rest[1].shape[2] <= LANES
        and own_rows % 16 == 0
        and feat % LANES == 0
        and gate_up_weight.shape[2] % LANES == 0
    )
    return (fused if fits else plain)(tokens, gate_up_weight, *rest)


def solution(mesh):
    in_specs = (
        P(("grp", "exp"), "tp"),
        P("tp", None, "exp"),
        P("exp", "tp"),
        P("exp", "tp", None),
        P("exp", None, "tp"),
        P(("grp", "exp"), None),
        P(("grp", "exp"), None),
    )
    out_specs = P(("grp", "exp"), "tp")
    return jax.shard_map(local, mesh=mesh, in_specs=in_specs, out_specs=out_specs, check_vma=False)
```
